32 devices in a mesh: row: 4 (over y, x), col: 8 (over z, core).
Axes of the slice: x: 2, y: 2, z: 4, core: 2. Of those that a mesh axis runs over, the one named last changes fastest.
Arguments:
- rhs: float32 [12288, 128], P('row'), may hold values from -6 to 6
- factor: float32 [10240, 4096], P('row', 'col'), may hold values from -0.09375 to 0.09375
- inverses: float32 [2, 2048, 2048], P(None, 'col', 'row'), may hold values from -1 to 3, as said below
Outputs:
- solution: float32 [4096, 128], P('col')
- remaining: float32 [8192, 128], P('row')
The draws below stay inside these ranges and needn't reach their ends.
Inputs may be any that keep to these rules, and one draw needn't show every extreme that they name: Each inverses[k] is lower triangular in panel order with positive diagonal entries.
All inputs are finite; a program needn't handle non-finite values.
Results may differ from the reference program's by a relative error of at most 0.000068.
Values sent between devices are 32-bit elements; how exact they have to be, the bound alone decides.
A program may use at most 64 MiB of HBM per device.

```python
import math
import jax
import jax.numpy as jnp
from jax import lax

PANEL = 2048
DENSITIES = 128
TRAIL_DEV = 2048
BLOCK_ROW = 512
BLOCK_COL = 256
TRAIL = 8192
N_ROW = 4
N_COL = 8


def draw_inverses(key, part):
    key_low, key_diag = jax.random.split(jax.random.fold_in(key, 17))
    lower = jax.random.truncated_normal(key_low, -4.0, 4.0, (2, PANEL, PANEL), jnp.float32) * (1.5 / math.sqrt(PANEL))
    diagonal = jax.random.uniform(key_diag, (2, PANEL), jnp.float32, 0.5, 1.5)
    return jnp.tril(lower, -1) + diagonal[:, :, None] * jnp.eye(PANEL, dtype=jnp.float32)


def shard_levels(rng, dims, cuts, smallest, largest):
    gain, own = 1.0, jax.random.fold_in(rng, 6)
    for position, shards_of in cuts:
        steps = jnp.exp(jax.random.uniform(jax.random.fold_in(own, position), (shards_of,), jnp.float32, smallest / len(cuts), largest / len(cuts)))
        gain = gain * jnp.repeat(steps, dims[position] // shards_of).reshape([-1 if axis == position else 1 for axis in range(len(dims))])
    return gain


def bell_draw(stream_key, dims, deviation, bound, pieces=(), kind=jnp.bfloat16):
    level = shard_levels(stream_key, dims, pieces, -0.22, 0.18) if pieces else 1.0
    drawn = jax.random.normal(stream_key, dims, jnp.float32) * deviation * level
    return jnp.minimum(jnp.maximum(drawn, -bound), bound).astype(kind)


def setup_inputs(seed: int = 0) -> dict:
    arg_keys = jax.random.split(jax.random.key(seed), 4)
    return {
        "rhs": bell_draw(arg_keys[0], (2 * PANEL + TRAIL, DENSITIES), 1.0, 6.0, ((0, 4),), jnp.float32),
        "factor": bell_draw(arg_keys[1], (PANEL + TRAIL, 2 * PANEL), (2 * PANEL) ** -0.5, 0.09375, ((0, 4), (1, 8)), jnp.float32),
        "inverses": draw_inverses(jax.random.fold_in(arg_keys[3], 71), 0),
    }


def product(left, right):
    return jnp.dot(left, right, precision=lax.Precision.HIGHEST, preferred_element_type=jnp.float32)


def reference(rhs, factor, inverses):
    rhs_blocks = rhs.reshape(N_ROW, 2 * BLOCK_ROW + TRAIL_DEV, DENSITIES)
    first_rhs = rhs_blocks[:, :BLOCK_ROW].reshape(PANEL, DENSITIES)
    second_rhs = rhs_blocks[:, BLOCK_ROW:2 * BLOCK_ROW].reshape(PANEL, DENSITIES)
    trailing = rhs_blocks[:, 2 * BLOCK_ROW:].reshape(TRAIL, DENSITIES)
    factor_blocks = factor.reshape(N_ROW, BLOCK_ROW + TRAIL_DEV, N_COL, 2, BLOCK_COL)
    first_cols = factor_blocks[:, :, :, 0, :].reshape(N_ROW, BLOCK_ROW + TRAIL_DEV, PANEL)
    second_cols = factor_blocks[:, :, :, 1, :].reshape(N_ROW, BLOCK_ROW + TRAIL_DEV, PANEL)
    coupling = first_cols[:, :BLOCK_ROW].reshape(PANEL, PANEL)
    trail_first = first_cols[:, BLOCK_ROW:].reshape(TRAIL, PANEL)
    trail_second = second_cols[:, BLOCK_ROW:].reshape(TRAIL, PANEL)
    first_sol = product(inverses[0], first_rhs)
    reduced = second_rhs - product(coupling, first_sol)
    second_sol = product(inverses[1], reduced)
    remaining = trailing - product(trail_first, first_sol) - product(trail_second, second_sol)
    solution = jnp.stack([first_sol.reshape(N_COL, BLOCK_COL, DENSITIES), second_sol.reshape(N_COL, BLOCK_COL, DENSITIES)], 1)
    return solution.reshape(2 * PANEL, DENSITIES), remaining
```

```python
import functools

import jax
import jax.numpy as jnp
from jax import lax
from jax.experimental import pallas as pl
from jax.experimental.pallas import tpu as pltpu
from jax.sharding import PartitionSpec as P

MESH = pl.DeviceIdType.MESH


def halves(x):
    high = x.astype(jnp.bfloat16)
    return high, (x - high.astype(jnp.float32)).astype(jnp.bfloat16)


def product(left, right):
    (lh, ll), (rh, rl) = left, right
    dot = functools.partial(jnp.dot, preferred_element_type=jnp.float32)
    return dot(lh, rh) + (dot(lh, rl) + dot(ll, rh))


def kernel(n_row, n_col, n_mid, n_end, skew_mid, skew_end,
           rhs, factor, inverses, sol, rem,
           inv_v, rhs_v, coup_v, fac_v, sums, got, pair0, pair1, red,
           mid_p, mid_rr, mid_rl, mid_sr, mid_sl,
           end_p, end_rr, end_rl, end_sr, end_sl, fac_h, fac_l,
           load_sem, swap_send, swap_recv, row_send, row_recv,
           mid_send, mid_recv, end_send, end_recv):
    span_rows = inv_v.shape[2]
    span_cols = inv_v.shape[1]
    half_r = span_rows // 2
    trail = rem.shape[0]
    half_t = trail // 2
    width = fac_v.shape[2]
    coup_w = coup_v.shape[2]
    phases = n_row.bit_length() - 1
    n_z = n_col // 2
    r = lax.axis_index("row")
    c = lax.axis_index("col")
    z, k = c // 2, c % 2
    mate = z * 2 + 1 - k

    def at(row, col):
        return {"row": row, "col": col}

    loads = [
        pltpu.make_async_copy(inverses.at[0], inv_v.at[0], load_sem.at[0]),
        pltpu.make_async_copy(rhs.at[pl.ds(0, span_rows)], rhs_v.at[pl.ds(0, span_rows)], load_sem.at[1]),
        pltpu.make_async_copy(factor.at[pl.ds(pl.multiple_of(k * half_r, 8), half_r), pl.ds(0, coup_w)], coup_v.at[k], load_sem.at[2]),
        pltpu.make_async_copy(inverses.at[1], inv_v.at[1], load_sem.at[3]),
        pltpu.make_async_copy(rhs.at[pl.ds(span_rows, span_rows + trail)], rhs_v.at[pl.ds(span_rows, span_rows + trail)], load_sem.at[4]),
        pltpu.make_async_copy(factor.at[pl.ds(pl.multiple_of(span_rows + k * half_t, 8), half_t)], fac_v.at[k], load_sem.at[5]),
    ]
    for load in loads:
        load.start()

    barrier = pltpu.get_barrier_semaphore()
    for p in range(phases):
        pl.semaphore_signal(barrier, inc=1, device_id=at(r ^ (1 << p), c), device_id_type=MESH)
    pl.semaphore_signal(barrier, inc=1, device_id=at(r, mate), device_id_type=MESH)

    @pl.when(z > 0)
    def _():
        pl.semaphore_signal(barrier, inc=1, device_id=at(r, c - 2), device_id_type=MESH)

    @pl.when(z < n_z - 1)
    def _():
        pl.semaphore_signal(barrier, inc=1, device_id=at(r, c + 2), device_id_type=MESH)

    cut = span_cols // 2

    def row_copy(panel, p, side):
        bit = p if side == 0 else phases - 1 - p
        return pltpu.make_async_remote_copy(
            src_ref=sums.at[panel, p, side], dst_ref=got.at[panel, p, side],
            send_sem=row_send.at[panel, p, side], recv_sem=row_recv.at[panel, p, side],
            device_id=at(r ^ (1 << bit), c), device_id_type=MESH)

    def row_finish(panel, pair, first_gap, later_gap):
        for p in range(phases):
            if p == 0:
                first_gap()
            elif p == 1:
                later_gap()
            for side in range(2):
                row_copy(panel, p, side).wait_recv()
                total = sums[panel, p, side] + got[panel, p, side]
                if p < phases - 1:
                    sums[panel, p + 1, side] = total
                    row_copy(panel, p + 1, side).start()
                else:
                    pair[k, pl.ds(side * cut, cut)] = total
                    sol[pl.ds(panel * span_cols + side * cut, cut)] = total

    def swap(i, src, dst):
        return pltpu.make_async_remote_copy(
            src_ref=src, dst_ref=dst, send_sem=swap_send.at[i], recv_sem=swap_recv.at[i],
            device_id=at(r, mate), device_id_type=MESH)

    def swap_coup():
        return swap(0, factor.at[pl.ds(pl.multiple_of((1 - k) * half_r, 8), half_r), pl.ds(0, coup_w)], coup_v.at[k])

    def swap_fac():
        return swap(1, factor.at[pl.ds(pl.multiple_of(span_rows + (1 - k) * half_t, 8), half_t)], fac_v.at[k])

    def swap_pair(i, pair):
        return swap(i, pair.at[k], pair.at[k])

    class Chain:
        def __init__(self, n, skew, part, rr, rl, sr, sl, send, recv, base, out):
            self.n, self.skew, self.part, self.rr, self.rl, self.sr, self.sl = n, skew, part, rr, rl, sr, sl
            self.send, self.recv, self.base, self.out = send, recv, base, out
            self.rows = part.shape[1]

        def copy(self, way, j, src):
            dst = self.rr if way == 0 else self.rl
            return pltpu.make_async_remote_copy(
                src_ref=src.at[j], dst_ref=dst.at[j], send_sem=self.send.at[way, j], recv_sem=self.recv.at[way, j],
                device_id=at(r, c + 2 if way == 0 else c - 2), device_id_type=MESH)

        def place(self, j, core):
            return pl.ds(pl.multiple_of((core * self.n + j) * self.rows, 8), self.rows)

        def cross(self, j):
            where = self.place(j, k)
            return pltpu.make_async_remote_copy(
                src_ref=self.out.at[where], dst_ref=self.out.at[where],
                send_sem=self.send.at[2, j], recv_sem=self.recv.at[2, j],
                device_id=at(r, mate), device_id_type=MESH)

        def launch(self, j):
            @pl.when(z == 0)
            def _():
                self.copy(0, j, self.part).start()

            @pl.when(z == n_z - 1)
            def _():
                self.copy(1, j, self.part).start()

        def run(self):
            inner = (z > 0) & (z < n_z - 1)
            off_r = jnp.where(inner, jnp.maximum(0, self.skew * (2 * z - n_z + 1)), 0)
            off_l = jnp.where(inner, jnp.maximum(0, self.skew * (n_z - 1 - 2 * z)), 0)
            off_f = jnp.maximum(off_r, off_l)

            def step(t, carry):
                jr, jl, jf = t - off_r, t - off_l, t - off_f

                @pl.when((z > 0) & (jr >= 0) & (jr < self.n))
                def _():
                    self.copy(0, jr, self.sr).wait_recv()
                    self.sr[jr] = self.rr[jr] + self.part[jr]

                    @pl.when(z < n_z - 1)
                    def _():
                        self.copy(0, jr, self.sr).start()

                @pl.when((z < n_z - 1) & (jl >= 0) & (jl < self.n))
                def _():
                    self.copy(1, jl, self.sl).wait_recv()
                    self.sl[jl] = self.rl[jl] + self.part[jl]

                    @pl.when(z > 0)
                    def _():
                        self.copy(1, jl, self.sl).start()

                @pl.when((jf >= 0) & (jf < self.n))
                def _():
                    first = rhs_v[pl.ds(pl.multiple_of(self.base + (k * self.n + jf) * self.rows, 8), self.rows)]
                    where = self.place(jf, k)

                    @pl.when(z == 0)
                    def _():
                        self.out[where] = first - self.sl[jf]

                    @pl.when(z == n_z - 1)
                    def _():
                        self.out[where] = first - self.sr[jf]

                    @pl.when(inner)
                    def _():
                        self.out[where] = first - (self.sr[jf] + self.rl[jf])

                    self.cross(jf).start()

                return carry

            lax.fori_loop(0, self.n + self.skew * max(n_z - 3, 0), step, 0)

            def gather(j, carry):
                self.cross(j).wait_recv()
                return carry

            lax.fori_loop(0, self.n, gather, 0)

        def drain(self):
            def step(j, carry):
                self.cross(j).wait_send()

                @pl.when(z < n_z - 1)
                def _():
                    self.copy(0, j, self.sr).wait_send()

                @pl.when(z > 0)
                def _():
                    self.copy(1, j, self.sl).wait_send()

                return carry

            lax.fori_loop(0, self.n, step, 0)

    mid = Chain(n_mid, skew_mid, mid_p, mid_rr, mid_rl, mid_sr, mid_sl, mid_send, mid_recv, span_rows, red)
    end = Chain(n_end, skew_end, end_p, end_rr, end_rl, end_sr, end_sl, end_send, end_recv, 2 * span_rows, rem)

    loads[0].wait()
    loads[1].wait()
    right = halves(rhs_v[pl.ds(0, span_rows)])
    for side in range(2):
        sums[0, 0, side] = product(halves(inv_v[0, pl.ds(side * cut, cut)]), right)
    pl.semaphore_wait(barrier, phases + 1 + (z > 0).astype(jnp.int32) + (z < n_z - 1).astype(jnp.int32))
    for side in range(2):
        row_copy(0, 0, side).start()

    def nothing():
        pass

    row_finish(0, pair0, lambda: swap_coup().start(), nothing)
    swap_pair(2, pair0).start()

    loads[2].wait()
    swap_coup().wait_recv()
    swap_pair(2, pair0).wait_recv()
    both0 = [halves(pair0[i]) for i in range(2)]
    for j in range(n_mid):
        rows = pl.ds(j * mid.rows, mid.rows)
        mid_p[j] = product(halves(coup_v[0, rows, :span_cols]), both0[0]) + product(halves(coup_v[1, rows, :span_cols]), both0[1])
        mid.launch(j)
    loads[3].wait()
    loads[4].wait()
    loads[5].wait()
    swap_fac().start()
    mid.run()

    right = halves(red[...])
    for side in range(2):
        sums[1, 0, side] = product(halves(inv_v[1, pl.ds(side * cut, cut)]), right)
        row_copy(1, 0, side).start()

    def carried():
        swap_fac().wait_recv()

        def step(j, carry):
            rows = pl.ds(pl.multiple_of(j * end.rows, 8), end.rows)
            end_p[j] = (product(halves(fac_v[0, rows, :span_cols]), halves(pair0[0]))
                        + product(halves(fac_v[1, rows, :span_cols]), halves(pair0[1])))
            return carry

        lax.fori_loop(0, n_end, step, 0)

    def split():
        def step(j, carry):
            rows = pl.ds(pl.multiple_of(j * end.rows, 16), end.rows)
            for i in range(2):
                fac_h[i, rows], fac_l[i, rows] = halves(fac_v[i, rows, span_cols:])
            return carry

        lax.fori_loop(0, n_end, step, 0)

    row_finish(1, pair1, carried, split)
    swap_pair(3, pair1).start()
    swap_pair(3, pair1).wait_recv()

    both1 = [halves(pair1[i]) for i in range(2)]

    def last(j, carry):
        rows = pl.ds(pl.multiple_of(j * end.rows, 16), end.rows)
        end_p[j] = end_p[j] + (product((fac_h[0, rows], fac_l[0, rows]), both1[0])
                               + product((fac_h[1, rows], fac_l[1, rows]), both1[1]))
        end.launch(j)
        return carry

    lax.fori_loop(0, n_end, last, 0)
    end.run()

    mid.drain()
    end.drain()
    swap_coup().wait_send()
    swap_fac().wait_send()
    swap_pair(2, pair0).wait_send()
    swap_pair(3, pair1).wait_send()
    for panel in range(2):
        for p in range(phases):
            for side in range(2):
                row_copy(panel, p, side).wait_send()


def local(n_row, n_col, rhs, factor, inverses):
    span_cols, span_rows = inverses.shape[1:]
    width = factor.shape[1]
    dens = rhs.shape[1]
    trail = rhs.shape[0] - 2 * span_rows
    phases = n_row.bit_length() - 1
    half_r, half_t = span_rows // 2, trail // 2
    coup_w = min(width, -(-span_cols // 128) * 128)
    n_mid = min(8, half_r // 8)
    n_end = min(16, half_t // 16)
    f32 = jnp.float32

    def chain_bufs(n, half):
        return [pltpu.VMEM((n, half // n, dens), f32)] * 5

    scratch = [
        pltpu.VMEM(inverses.shape, f32),
        pltpu.VMEM(rhs.shape, f32),
        pltpu.VMEM((2, half_r, coup_w), f32),
        pltpu.VMEM((2, half_t, width), f32),
        pltpu.VMEM((2, phases, 2, span_cols // 2, dens), f32),
        pltpu.VMEM((2, phases, 2, span_cols // 2, dens), f32),
        pltpu.VMEM((2, span_cols, dens), f32),
        pltpu.VMEM((2, span_cols, dens), f32),
        pltpu.VMEM((span_rows, dens), f32),
        *chain_bufs(n_mid, half_r),
        *chain_bufs(n_end, half_t),
        pltpu.VMEM((2, half_t, span_cols), jnp.bfloat16),
        pltpu.VMEM((2, half_t, span_cols), jnp.bfloat16),
        pltpu.SemaphoreType.DMA((6,)),
        pltpu.SemaphoreType.DMA((4,)),
        pltpu.SemaphoreType.DMA((4,)),
        pltpu.SemaphoreType.DMA((2, phases, 2)),
        pltpu.SemaphoreType.DMA((2, phases, 2)),
        pltpu.SemaphoreType.DMA((3, n_mid)),
        pltpu.SemaphoreType.DMA((3, n_mid)),
        pltpu.SemaphoreType.DMA((3, n_end)),
        pltpu.SemaphoreType.DMA((3, n_end)),
    ]
    return pl.pallas_call(
        functools.partial(kernel, n_row, n_col, n_mid, n_end, 4, 3),
        out_shape=(jax.ShapeDtypeStruct((2 * span_cols, dens), f32), jax.ShapeDtypeStruct((trail, dens), f32)),
        in_specs=[pl.BlockSpec(memory_space=pl.ANY)] * 3,
        out_specs=(pl.BlockSpec(memory_space=pltpu.VMEM), pl.BlockSpec(memory_space=pltpu.VMEM)),
        scratch_shapes=scratch,
        compiler_params=pltpu.CompilerParams(collective_id=0, has_side_effects=True),
    )(rhs, factor, inverses)


def solution(mesh):
    in_specs = (P("row", None), P("row", "col"), P(None, "col", "row"))
    out_specs = (P("col", None), P("row", None))
    body = functools.partial(local, mesh.shape["row"], mesh.shape["col"])
    return jax.shard_map(body, mesh=mesh, in_specs=in_specs, out_specs=out_specs, check_vma=False)
```

```python
import functools

import jax
import jax.numpy as jnp
from jax import lax
from jax.experimental import pallas as pl
from jax.experimental.pallas import tpu as pltpu
from jax.sharding import PartitionSpec as P

MESH = pl.DeviceIdType.MESH


def halves(x):
    high = x.astype(jnp.bfloat16)
    return high, (x - high.astype(jnp.float32)).astype(jnp.bfloat16)


def product(left, right):
    (lh, ll), (rh, rl) = left, right
    dot = functools.partial(jnp.dot, preferred_element_type=jnp.float32)
    return dot(lh, rh) + (dot(lh, rl) + dot(ll, rh))


def kernel(n_row, n_col, n_mid, n_end, skew_mid, skew_end,
           rhs, factor, inverses, sol, rem,
           inv_v, rhs_v, coup_v, fac_v, sums, got, pair0, pair1, red,
           mid_p, mid_rr, mid_rl, mid_sr, mid_sl,
           end_p, end_rr, end_rl, end_sr, end_sl, fac_h, fac_l,
           load_sem, swap_send, swap_recv, row_send, row_recv,
           mid_send, mid_recv, end_send, end_recv):
    span_rows = inv_v.shape[2]
    span_cols = inv_v.shape[1]
    half_r = span_rows // 2
    trail = rem.shape[0]
    half_t = trail // 2
    width = fac_v.shape[2]
    coup_w = coup_v.shape[2]
    phases = n_row.bit_length() - 1
    n_z = n_col // 2
    r = lax.axis_index("row")
    c = lax.axis_index("col")
    z, k = c // 2, c % 2
    mate = z * 2 + 1 - k

    def at(row, col):
        return {"row": row, "col": col}

    loads = [
        pltpu.make_async_copy(inverses.at[0], inv_v.at[0], load_sem.at[0]),
        pltpu.make_async_copy(rhs.at[pl.ds(0, span_rows)], rhs_v.at[pl.ds(0, span_rows)], load_sem.at[1]),
        pltpu.make_async_copy(factor.at[pl.ds(pl.multiple_of(k * half_r, 8), half_r), pl.ds(0, coup_w)], coup_v.at[k], load_sem.at[2]),
        pltpu.make_async_copy(inverses.at[1], inv_v.at[1], load_sem.at[3]),
        pltpu.make_async_copy(rhs.at[pl.ds(span_rows, span_rows + trail)], rhs_v.at[pl.ds(span_rows, span_rows + trail)], load_sem.at[4]),
        pltpu.make_async_copy(factor.at[pl.ds(pl.multiple_of(span_rows + k * half_t, 8), half_t)], fac_v.at[k], load_sem.at[5]),
    ]
    for load in loads[:2]:
        load.start()

    barrier = pltpu.get_barrier_semaphore()
    for p in range(phases):
        pl.semaphore_signal(barrier, inc=1, device_id=at(r ^ (1 << p), c), device_id_type=MESH)
    pl.semaphore_signal(barrier, inc=1, device_id=at(r, mate), device_id_type=MESH)

    @pl.when(z > 0)
    def _():
        pl.semaphore_signal(barrier, inc=1, device_id=at(r, c - 2), device_id_type=MESH)

    @pl.when(z < n_z - 1)
    def _():
        pl.semaphore_signal(barrier, inc=1, device_id=at(r, c + 2), device_id_type=MESH)

    pieces = sums.shape[2]
    cut = span_cols // pieces

    def row_copy(panel, p, side):
        bit = p if side % 2 == 0 else phases - 1 - p
        return pltpu.make_async_remote_copy(
            src_ref=sums.at[panel, p, side], dst_ref=got.at[panel, p, side],
            send_sem=row_send.at[panel, p, side], recv_sem=row_recv.at[panel, p, side],
            device_id=at(r ^ (1 << bit), c), device_id_type=MESH)

    def row_finish(panel, pair, first_gap, later_gap):
        for p in range(phases):
            if p == 0:
                first_gap()
            elif p == 1:
                later_gap()
            for side in range(pieces):
                row_copy(panel, p, side).wait_recv()
                total = sums[panel, p, side] + got[panel, p, side]
                if p < phases - 1:
                    sums[panel, p + 1, side] = total
                    row_copy(panel, p + 1, side).start()
                else:
                    pair[k, pl.ds(side * cut, cut)] = total
                    sol[pl.ds(panel * span_cols + side * cut, cut)] = total

    def swap(i, src, dst):
        return pltpu.make_async_remote_copy(
            src_ref=src, dst_ref=dst, send_sem=swap_send.at[i], recv_sem=swap_recv.at[i],
            device_id=at(r, mate), device_id_type=MESH)

    def swap_coup():
        return swap(0, factor.at[pl.ds(pl.multiple_of((1 - k) * half_r, 8), half_r), pl.ds(0, coup_w)], coup_v.at[k])

    def swap_fac():
        return swap(1, factor.at[pl.ds(pl.multiple_of(span_rows + (1 - k) * half_t, 8), half_t)], fac_v.at[k])

    def swap_pair(i, pair):
        return swap(i, pair.at[k], pair.at[k])

    class Chain:
        def __init__(self, n, skew, part, rr, rl, sr, sl, send, recv, base, out):
            self.n, self.skew, self.part, self.rr, self.rl, self.sr, self.sl = n, skew, part, rr, rl, sr, sl
            self.send, self.recv, self.base, self.out = send, recv, base, out
            self.rows = part.shape[1]

        def copy(self, way, j, src):
            dst = self.rr if way == 0 else self.rl
            return pltpu.make_async_remote_copy(
                src_ref=src.at[j], dst_ref=dst.at[j], send_sem=self.send.at[way, j], recv_sem=self.recv.at[way, j],
                device_id=at(r, c + 2 if way == 0 else c - 2), device_id_type=MESH)

        def place(self, j, core):
            return pl.ds(pl.multiple_of((core * self.n + j) * self.rows, 8), self.rows)

        def cross(self, j):
            where = self.place(j, k)
            return pltpu.make_async_remote_copy(
                src_ref=self.out.at[where], dst_ref=self.out.at[where],
                send_sem=self.send.at[2, j], recv_sem=self.recv.at[2, j],
                device_id=at(r, mate), device_id_type=MESH)

        def launch(self, j):
            @pl.when(z == 0)
            def _():
                self.copy(0, j, self.part).start()

            @pl.when(z == n_z - 1)
            def _():
                self.copy(1, j, self.part).start()

        def run(self):
            inner = (z > 0) & (z < n_z - 1)
            off_r = jnp.where(inner, jnp.maximum(0, self.skew * (2 * z - n_z + 1)), 0)
            off_l = jnp.where(inner, jnp.maximum(0, self.skew * (n_z - 1 - 2 * z)), 0)
            off_f = jnp.maximum(off_r, off_l)

            def step(t, carry):
                jr, jl, jf = t - off_r, t - off_l, t - off_f

                @pl.when((z > 0) & (jr >= 0) & (jr < self.n))
                def _():
                    self.copy(0, jr, self.sr).wait_recv()
                    self.sr[jr] = self.rr[jr] + self.part[jr]

                    @pl.when(z < n_z - 1)
                    def _():
                        self.copy(0, jr, self.sr).start()

                @pl.when((z < n_z - 1) & (jl >= 0) & (jl < self.n))
                def _():
                    self.copy(1, jl, self.sl).wait_recv()
                    self.sl[jl] = self.rl[jl] + self.part[jl]

                    @pl.when(z > 0)
                    def _():
                        self.copy(1, jl, self.sl).start()

                @pl.when((jf >= 0) & (jf < self.n))
                def _():
                    first = rhs_v[pl.ds(pl.multiple_of(self.base + (k * self.n + jf) * self.rows, 8), self.rows)]
                    where = self.place(jf, k)

                    @pl.when(z == 0)
                    def _():
                        self.out[where] = first - self.sl[jf]

                    @pl.when(z == n_z - 1)
                    def _():
                        self.out[where] = first - self.sr[jf]

                    @pl.when(inner)
                    def _():
                        self.out[where] = first - (self.sr[jf] + self.rl[jf])

                    self.cross(jf).start()

                return carry

            lax.fori_loop(0, self.n + self.skew * max(n_z - 3, 0), step, 0)

            def gather(j, carry):
                self.cross(j).wait_recv()
                return carry

            lax.fori_loop(0, self.n, gather, 0)

        def drain(self):
            def step(j, carry):
                self.cross(j).wait_send()

                @pl.when(z < n_z - 1)
                def _():
                    self.copy(0, j, self.sr).wait_send()

                @pl.when(z > 0)
                def _():
                    self.copy(1, j, self.sl).wait_send()

                return carry

            lax.fori_loop(0, self.n, step, 0)

    mid = Chain(n_mid, skew_mid, mid_p, mid_rr, mid_rl, mid_sr, mid_sl, mid_send, mid_recv, span_rows, red)
    end = Chain(n_end, skew_end, end_p, end_rr, end_rl, end_sr, end_sl, end_send, end_recv, 2 * span_rows, rem)

    loads[0].wait()
    loads[1].wait()
    for load in loads[2:]:
        load.start()
    right = halves(rhs_v[pl.ds(0, span_rows)])
    for side in range(pieces):
        sums[0, 0, side] = product(halves(inv_v[0, pl.ds(side * cut, cut)]), right)
    pl.semaphore_wait(barrier, phases + 1 + (z > 0).astype(jnp.int32) + (z < n_z - 1).astype(jnp.int32))
    for side in range(pieces):
        row_copy(0, 0, side).start()

    def nothing():
        pass

    row_finish(0, pair0, lambda: swap_coup().start(), nothing)
    swap_pair(2, pair0).start()

    loads[2].wait()
    swap_coup().wait_recv()
    swap_pair(2, pair0).wait_recv()
    both0 = [halves(pair0[i]) for i in range(2)]
    for j in range(n_mid):
        rows = pl.ds(j * mid.rows, mid.rows)
        mid_p[j] = product(halves(coup_v[0, rows, :span_cols]), both0[0]) + product(halves(coup_v[1, rows, :span_cols]), both0[1])
        mid.launch(j)
    loads[3].wait()
    loads[4].wait()
    loads[5].wait()
    swap_fac().start()
    mid.run()

    right = halves(red[...])
    for side in range(pieces):
        sums[1, 0, side] = product(halves(inv_v[1, pl.ds(side * cut, cut)]), right)
        row_copy(1, 0, side).start()

    def carried():
        swap_fac().wait_recv()

        def step(j, carry):
            rows = pl.ds(pl.multiple_of(j * end.rows, 8), end.rows)
            end_p[j] = (product(halves(fac_v[0, rows, :span_cols]), halves(pair0[0]))
                        + product(halves(fac_v[1, rows, :span_cols]), halves(pair0[1])))
            return carry

        lax.fori_loop(0, n_end, step, 0)

    def split():
        def step(j, carry):
            rows = pl.ds(pl.multiple_of(j * end.rows, 16), end.rows)
            for i in range(2):
                fac_h[i, rows], fac_l[i, rows] = halves(fac_v[i, rows, span_cols:])
            return carry

        lax.fori_loop(0, n_end, step, 0)

    row_finish(1, pair1, carried, split)
    swap_pair(3, pair1).start()
    swap_pair(3, pair1).wait_recv()

    both1 = [halves(pair1[i]) for i in range(2)]

    def last(j, carry):
        rows = pl.ds(pl.multiple_of(j * end.rows, 16), end.rows)
        end_p[j] = end_p[j] + (product((fac_h[0, rows], fac_l[0, rows]), both1[0])
                               + product((fac_h[1, rows], fac_l[1, rows]), both1[1]))
        end.launch(j)
        return carry

    lax.fori_loop(0, n_end, last, 0)
    end.run()

    mid.drain()
    end.drain()
    swap_coup().wait_send()
    swap_fac().wait_send()
    swap_pair(2, pair0).wait_send()
    swap_pair(3, pair1).wait_send()
    for panel in range(2):
        for p in range(phases):
            for side in range(pieces):
                row_copy(panel, p, side).wait_send()


def local(n_row, n_col, rhs, factor, inverses):
    span_cols, span_rows = inverses.shape[1:]
    width = factor.shape[1]
    dens = rhs.shape[1]
    trail = rhs.shape[0] - 2 * span_rows
    phases = n_row.bit_length() - 1
    half_r, half_t = span_rows // 2, trail // 2
    coup_w = min(width, -(-span_cols // 128) * 128)
    n_mid = min(8, half_r // 8)
    n_end = min(8, half_t // 16)
    pieces = 4
    f32 = jnp.float32

    def chain_bufs(n, half):
        return [pltpu.VMEM((n, half // n, dens), f32)] * 5

    scratch = [
        pltpu.VMEM(inverses.shape, f32),
        pltpu.VMEM(rhs.shape, f32),
        pltpu.VMEM((2, half_r, coup_w), f32),
        pltpu.VMEM((2, half_t, width), f32),
        pltpu.VMEM((2, phases, pieces, span_cols // pieces, dens), f32),
        pltpu.VMEM((2, phases, pieces, span_cols // pieces, dens), f32),
        pltpu.VMEM((2, span_cols, dens), f32),
        pltpu.VMEM((2, span_cols, dens), f32),
        pltpu.VMEM((span_rows, dens), f32),
        *chain_bufs(n_mid, half_r),
        *chain_bufs(n_end, half_t),
        pltpu.VMEM((2, half_t, span_cols), jnp.bfloat16),
        pltpu.VMEM((2, half_t, span_cols), jnp.bfloat16),
        pltpu.SemaphoreType.DMA((6,)),
        pltpu.SemaphoreType.DMA((4,)),
        pltpu.SemaphoreType.DMA((4,)),
        pltpu.SemaphoreType.DMA((2, phases, pieces)),
        pltpu.SemaphoreType.DMA((2, phases, pieces)),
        pltpu.SemaphoreType.DMA((3, n_mid)),
        pltpu.SemaphoreType.DMA((3, n_mid)),
        pltpu.SemaphoreType.DMA((3, n_end)),
        pltpu.SemaphoreType.DMA((3, n_end)),
    ]
    return pl.pallas_call(
        functools.partial(kernel, n_row, n_col, n_mid, n_end, 5, 2),
        out_shape=(pltpu.VMEM((2 * span_cols, dens), f32), pltpu.VMEM((trail, dens), f32)),
        in_specs=[pl.BlockSpec(memory_space=pl.ANY)] * 3,
        out_specs=(pl.BlockSpec(memory_space=pltpu.VMEM), pl.BlockSpec(memory_space=pltpu.VMEM)),
        scratch_shapes=scratch,
        compiler_params=pltpu.CompilerParams(collective_id=0, has_side_effects=True),
    )(rhs, factor, inverses)


def solution(mesh):
    in_specs = (P("row", None), P("row", "col"), P(None, "col", "row"))
    out_specs = (P("col", None), P("row", None))
    body = functools.partial(local, mesh.shape["row"], mesh.shape["col"])
    return jax.shard_map(body, mesh=mesh, in_specs=in_specs, out_specs=out_specs, check_vma=False)
```

```python
import functools

import jax
import jax.numpy as jnp
from jax import lax
from jax.experimental import pallas as pl
from jax.experimental.pallas import tpu as pltpu
from jax.sharding import PartitionSpec as P

MESH = pl.DeviceIdType.MESH


def halves(x):
    high = x.astype(jnp.bfloat16)
    return high, (x - high.astype(jnp.float32)).astype(jnp.bfloat16)


def product(left, right):
    (lh, ll), (rh, rl) = left, right
    dot = functools.partial(jnp.dot, preferred_element_type=jnp.float32)
    return dot(lh, rh) + (dot(lh, rl) + dot(ll, rh))


def kernel(n_row, n_col, n_mid, n_end, skew_mid, skew_end,
           rhs, factor, inverses, sol, rem,
           inv_v, rhs_v, coup_v, fac_v, sums, got, pair0, pair1, red,
           mid_p, mid_rr, mid_rl, mid_sr, mid_sl,
           end_p, end_rr, end_rl, end_sr, end_sl, fac_h, fac_l,
           load_sem, swap_send, swap_recv, row_send, row_recv,
           mid_send, mid_recv, end_send, end_recv):
    span_rows = inv_v.shape[2]
    span_cols = inv_v.shape[1]
    half_r = span_rows // 2
    trail = rem.shape[0]
    half_t = trail // 2
    width = fac_v.shape[2]
    coup_w = coup_v.shape[2]
    phases = n_row.bit_length() - 1
    n_z = n_col // 2
    r = lax.axis_index("row")
    c = lax.axis_index("col")
    z, k = c // 2, c % 2
    mate = z * 2 + 1 - k

    def at(row, col):
        return {"row": row, "col": col}

    loads = [
        pltpu.make_async_copy(inverses.at[0], inv_v.at[0], load_sem.at[0]),
        pltpu.make_async_copy(rhs.at[pl.ds(0, span_rows)], rhs_v.at[pl.ds(0, span_rows)], load_sem.at[1]),
        pltpu.make_async_copy(factor.at[pl.ds(pl.multiple_of(k * half_r, 8), half_r), pl.ds(0, coup_w)], coup_v.at[k], load_sem.at[2]),
        pltpu.make_async_copy(inverses.at[1], inv_v.at[1], load_sem.at[3]),
        pltpu.make_async_copy(rhs.at[pl.ds(span_rows, span_rows + trail)], rhs_v.at[pl.ds(span_rows, span_rows + trail)], load_sem.at[4]),
        pltpu.make_async_copy(factor.at[pl.ds(pl.multiple_of(span_rows + k * half_t, 8), half_t)], fac_v.at[k], load_sem.at[5]),
    ]
    for load in loads[:2]:
        load.start()

    barrier = pltpu.get_barrier_semaphore()
    for p in range(phases):
        pl.semaphore_signal(barrier, inc=1, device_id=at(r ^ (1 << p), c), device_id_type=MESH)
    pl.semaphore_signal(barrier, inc=1, device_id=at(r, mate), device_id_type=MESH)

    @pl.when(z > 0)
    def _():
        pl.semaphore_signal(barrier, inc=1, device_id=at(r, c - 2), device_id_type=MESH)

    @pl.when(z < n_z - 1)
    def _():
        pl.semaphore_signal(barrier, inc=1, device_id=at(r, c + 2), device_id_type=MESH)

    pieces = sums.shape[2]
    cut = span_cols // pieces

    def row_copy(panel, p, side):
        bit = p if side % 2 == 0 else phases - 1 - p
        return pltpu.make_async_remote_copy(
            src_ref=sums.at[panel, p, side], dst_ref=got.at[panel, p, side],
            send_sem=row_send.at[panel, p, side], recv_sem=row_recv.at[panel, p, side],
            device_id=at(r ^ (1 << bit), c), device_id_type=MESH)

    def row_finish(panel, pair, first_gap, later_gap):
        for p in range(phases):
            if p == 0:
                first_gap()
            elif p == 1:
                later_gap()
            for side in range(pieces):
                row_copy(panel, p, side).wait_recv()
                total = sums[panel, p, side] + got[panel, p, side]
                if p < phases - 1:
                    sums[panel, p + 1, side] = total
                    row_copy(panel, p + 1, side).start()
                else:
                    pair[k, pl.ds(side * cut, cut)] = total
                    sol[pl.ds(panel * span_cols + side * cut, cut)] = total

    def swap(i, src, dst):
        return pltpu.make_async_remote_copy(
            src_ref=src, dst_ref=dst, send_sem=swap_send.at[i], recv_sem=swap_recv.at[i],
            device_id=at(r, mate), device_id_type=MESH)

    def swap_coup():
        return swap(0, factor.at[pl.ds(pl.multiple_of((1 - k) * half_r, 8), half_r), pl.ds(0, coup_w)], coup_v.at[k])

    def swap_fac():
        return swap(1, factor.at[pl.ds(pl.multiple_of(span_rows + (1 - k) * half_t, 8), half_t)], fac_v.at[k])

    def swap_pair(i, pair):
        return swap(i, pair.at[k], pair.at[k])

    class Chain:
        def __init__(self, n, skew, part, rr, rl, sr, sl, send, recv, base, out):
            self.n, self.skew, self.part, self.rr, self.rl, self.sr, self.sl = n, skew, part, rr, rl, sr, sl
            self.send, self.recv, self.base, self.out = send, recv, base, out
            self.rows = part.shape[1]

        def copy(self, way, j, src):
            dst = self.rr if way == 0 else self.rl
            return pltpu.make_async_remote_copy(
                src_ref=src.at[j], dst_ref=dst.at[j], send_sem=self.send.at[way, j], recv_sem=self.recv.at[way, j],
                device_id=at(r, c + 2 if way == 0 else c - 2), device_id_type=MESH)

        def place(self, j, core):
            return pl.ds(pl.multiple_of((core * self.n + j) * self.rows, 8), self.rows)

        def cross(self, j):
            where = self.place(j, k)
            return pltpu.make_async_remote_copy(
                src_ref=self.out.at[where], dst_ref=self.out.at[where],
                send_sem=self.send.at[2, j], recv_sem=self.recv.at[2, j],
                device_id=at(r, mate), device_id_type=MESH)

        def launch(self, j):
            @pl.when(z == 0)
            def _():
                self.copy(0, j, self.part).start()

            @pl.when(z == n_z - 1)
            def _():
                self.copy(1, j, self.part).start()

        def run(self):
            inner = (z > 0) & (z < n_z - 1)
            off_r = jnp.where(inner, jnp.maximum(0, self.skew * (2 * z - n_z + 1)), 0)
            off_l = jnp.where(inner, jnp.maximum(0, self.skew * (n_z - 1 - 2 * z)), 0)
            off_f = jnp.maximum(off_r, off_l)

            def step(t, carry):
                jr, jl, jf = t - off_r, t - off_l, t - off_f

                @pl.when((z > 0) & (jr >= 0) & (jr < self.n))
                def _():
                    self.copy(0, jr, self.sr).wait_recv()
                    self.sr[jr] = self.rr[jr] + self.part[jr]

                    @pl.when(z < n_z - 1)
                    def _():
                        self.copy(0, jr, self.sr).start()

                @pl.when((z < n_z - 1) & (jl >= 0) & (jl < self.n))
                def _():
                    self.copy(1, jl, self.sl).wait_recv()
                    self.sl[jl] = self.rl[jl] + self.part[jl]

                    @pl.when(z > 0)
                    def _():
                        self.copy(1, jl, self.sl).start()

                @pl.when((jf >= 0) & (jf < self.n))
                def _():
                    first = rhs_v[pl.ds(pl.multiple_of(self.base + (k * self.n + jf) * self.rows, 8), self.rows)]
                    where = self.place(jf, k)

                    @pl.when(z == 0)
                    def _():
                        self.out[where] = first - self.sl[jf]

                    @pl.when(z == n_z - 1)
                    def _():
                        self.out[where] = first - self.sr[jf]

                    @pl.when(inner)
                    def _():
                        self.out[where] = first - (self.sr[jf] + self.rl[jf])

                    self.cross(jf).start()

                return carry

            lax.fori_loop(0, self.n + self.skew * max(n_z - 3, 0), step, 0)

            def gather(j, carry):
                self.cross(j).wait_recv()
                return carry

            lax.fori_loop(0, self.n, gather, 0)

        def drain(self):
            def step(j, carry):
                self.cross(j).wait_send()

                @pl.when(z < n_z - 1)
                def _():
                    self.copy(0, j, self.sr).wait_send()

                @pl.when(z > 0)
                def _():
                    self.copy(1, j, self.sl).wait_send()

                return carry

            lax.fori_loop(0, self.n, step, 0)

    mid = Chain(n_mid, skew_mid, mid_p, mid_rr, mid_rl, mid_sr, mid_sl, mid_send, mid_recv, span_rows, red)
    end = Chain(n_end, skew_end, end_p, end_rr, end_rl, end_sr, end_sl, end_send, end_recv, 2 * span_rows, rem)

    loads[0].wait()
    loads[1].wait()
    for load in loads[2:]:
        load.start()
    right = halves(rhs_v[pl.ds(0, span_rows)])
    total = product(halves(inv_v[0]), right)
    for side in range(pieces):
        sums[0, 0, side] = total[side * cut:(side + 1) * cut]
    pl.semaphore_wait(barrier, phases + 1 + (z > 0).astype(jnp.int32) + (z < n_z - 1).astype(jnp.int32))
    for side in range(pieces):
        row_copy(0, 0, side).start()

    def nothing():
        pass

    row_finish(0, pair0, lambda: swap_coup().start(), nothing)
    swap_pair(2, pair0).start()

    loads[2].wait()
    swap_coup().wait_recv()
    swap_pair(2, pair0).wait_recv()
    both0 = [halves(pair0[i]) for i in range(2)]
    total = product(halves(coup_v[0, :, :span_cols]), both0[0]) + product(halves(coup_v[1, :, :span_cols]), both0[1])
    for j in range(n_mid):
        mid_p[j] = total[j * mid.rows:(j + 1) * mid.rows]
        mid.launch(j)
    loads[3].wait()
    loads[4].wait()
    loads[5].wait()
    swap_fac().start()
    mid.run()

    right = halves(red[...])
    total = product(halves(inv_v[1]), right)
    for side in range(pieces):
        sums[1, 0, side] = total[side * cut:(side + 1) * cut]
        row_copy(1, 0, side).start()

    def carried():
        swap_fac().wait_recv()

        def step(j, carry):
            rows = pl.ds(pl.multiple_of(j * end.rows, 8), end.rows)
            end_p[j] = (product(halves(fac_v[0, rows, :span_cols]), halves(pair0[0]))
                        + product(halves(fac_v[1, rows, :span_cols]), halves(pair0[1])))
            return carry

        lax.fori_loop(0, n_end, step, 0)

    def split():
        def step(j, carry):
            rows = pl.ds(pl.multiple_of(j * end.rows, 16), end.rows)
            for i in range(2):
                fac_h[i, rows], fac_l[i, rows] = halves(fac_v[i, rows, span_cols:])
            return carry

        lax.fori_loop(0, n_end, step, 0)

    row_finish(1, pair1, carried, split)
    swap_pair(3, pair1).start()
    swap_pair(3, pair1).wait_recv()

    both1 = [halves(pair1[i]) for i in range(2)]

    group = max(1, n_end // 4)

    def last(j, carry):
        rows = pl.ds(pl.multiple_of(j * group * end.rows, 16), group * end.rows)
        total = (product((fac_h[0, rows], fac_l[0, rows]), both1[0])
                 + product((fac_h[1, rows], fac_l[1, rows]), both1[1]))
        for i in range(group):
            end_p[j * group + i] = end_p[j * group + i] + total[i * end.rows:(i + 1) * end.rows]
            end.launch(j * group + i)
        return carry

    lax.fori_loop(0, n_end // group, last, 0)
    end.run()

    mid.drain()
    end.drain()
    swap_coup().wait_send()
    swap_fac().wait_send()
    swap_pair(2, pair0).wait_send()
    swap_pair(3, pair1).wait_send()
    for panel in range(2):
        for p in range(phases):
            for side in range(pieces):
                row_copy(panel, p, side).wait_send()


def local(n_row, n_col, rhs, factor, inverses):
    span_cols, span_rows = inverses.shape[1:]
    width = factor.shape[1]
    dens = rhs.shape[1]
    trail = rhs.shape[0] - 2 * span_rows
    phases = n_row.bit_length() - 1
    half_r, half_t = span_rows // 2, trail // 2
    coup_w = min(width, -(-span_cols // 128) * 128)
    n_mid = min(4, half_r // 8)
    n_end = min(16, half_t // 16)
    pieces = 4
    f32 = jnp.float32

    def chain_bufs(n, half):
        return [pltpu.VMEM((n, half // n, dens), f32)] * 5

    scratch = [
        pltpu.VMEM(inverses.shape, f32),
        pltpu.VMEM(rhs.shape, f32),
        pltpu.VMEM((2, half_r, coup_w), f32),
        pltpu.VMEM((2, half_t, width), f32),
        pltpu.VMEM((2, phases, pieces, span_cols // pieces, dens), f32),
        pltpu.VMEM((2, phases, pieces, span_cols // pieces, dens), f32),
        pltpu.VMEM((2, span_cols, dens), f32),
        pltpu.VMEM((2, span_cols, dens), f32),
        pltpu.VMEM((span_rows, dens), f32),
        *chain_bufs(n_mid, half_r),
        *chain_bufs(n_end, half_t),
        pltpu.VMEM((2, half_t, span_cols), jnp.bfloat16),
        pltpu.VMEM((2, half_t, span_cols), jnp.bfloat16),
        pltpu.SemaphoreType.DMA((6,)),
        pltpu.SemaphoreType.DMA((4,)),
        pltpu.SemaphoreType.DMA((4,)),
        pltpu.SemaphoreType.DMA((2, phases, pieces)),
        pltpu.SemaphoreType.DMA((2, phases, pieces)),
        pltpu.SemaphoreType.DMA((3, n_mid)),
        pltpu.SemaphoreType.DMA((3, n_mid)),
        pltpu.SemaphoreType.DMA((3, n_end)),
        pltpu.SemaphoreType.DMA((3, n_end)),
    ]
    return pl.pallas_call(
        functools.partial(kernel, n_row, n_col, n_mid, n_end, 3, 4),
        out_shape=(pltpu.VMEM((2 * span_cols, dens), f32), pltpu.VMEM((trail, dens), f32)),
        in_specs=[pl.BlockSpec(memory_space=pl.ANY)] * 3,
        out_specs=(pl.BlockSpec(memory_space=pltpu.VMEM), pl.BlockSpec(memory_space=pltpu.VMEM)),
        scratch_shapes=scratch,
        compiler_params=pltpu.CompilerParams(collective_id=0, has_side_effects=True),
    )(rhs, factor, inverses)


def solution(mesh):
    in_specs = (P("row", None), P("row", "col"), P(None, "col", "row"))
    out_specs = (P("col", None), P("row", None))
    body = functools.partial(local, mesh.shape["row"], mesh.shape["col"])
    return jax.shard_map(body, mesh=mesh, in_specs=in_specs, out_specs=out_specs, check_vma=False)
```
